512 devices in a mesh: parts: 2 (over y), seq: 32 (over z), head: 8 (over x, core).
Axes of the slice: x: 4, y: 2, z: 32, core: 2. Of those that a mesh axis runs over, the one named last changes fastest.
The devices are a block of a 4x8x32 slice.
Arguments:
- hidden: bfloat16 [48, 12288], P(('parts', 'head'), 'seq'), parts along dimension 0, may hold values from -600 to 600
- norm_gain: float32 [12288], P('seq'), may hold values from 0.1 to 1.9
- w_query: bfloat16 [12288, 12288], P('seq', 'head'), may hold values from -0.0546875 to 0.0546875
- w_key: bfloat16 [12288, 1024], P('seq', 'head'), may hold values from -0.0546875 to 0.0546875
- w_value: bfloat16 [12288, 1024], P('seq', 'head'), may hold values from -0.0546875 to 0.0546875
- w_out: bfloat16 [12288, 12288], P('head', 'seq'), may hold values from -0.0546875 to 0.0546875
- lengths: int32 [48], P('parts'), parts along dimension 0, may hold values from 1 to 4096, as said below
- key_cache: bfloat16 [48, 8, 4096, 128], P('parts', 'head', 'seq'), parts along dimension 0, may hold values from -600 to 600, as said below
- value_cache: bfloat16 [48, 8, 4096, 128], P('parts', 'head', 'seq'), parts along dimension 0, may hold values from -6 to 6
Outputs:
- attn_out: bfloat16 [48, 12288], P(('parts', 'head'), 'seq'), parts along dimension 0
The draws below stay inside these ranges and needn't reach their ends.
There are 2 independent parts, one for each index of `parts`. The reference program is written for one: setup_inputs(seed, part) draws one part's arguments, and reference() takes and returns one part's arrays. A program takes and returns all parts, laid end to end along the dimension named above; an argument that names none is the same for every part. Nothing has to cross between parts.
Inputs may be any that keep to these rules, and one draw needn't show every extreme that they name: Sequence b holds lengths[b] cached tokens at positions 0 to lengths[b] - 1; its new token takes position lengths[b]. `key_cache`: positions at or past a sequence's length hold no data.
All inputs are finite; a program needn't handle non-finite values.
Results may differ from the reference program's by a relative error of at most 0.0075.
The reference program's roundings to bfloat16 on the way (of `scaled`, `queries`, `weights` and `mixed`) count: a program that leaves them out, or rounds other values in their place, can miss the bound.
Values may be sent and summed in bfloat16 or wider, within the bound.
No kernel may reach another device: no remote copies, remote signals or barrier semaphores. Data moves between devices by JAX's collectives and lax.ppermute only.
A program may use at most 64 MiB of HBM per device.

```python
import jax
import jax.numpy as jnp
from jax import lax

D = 12288
HEADS = 96
KV_HEADS = 8
HD = 128
BATCH = 24
CTX_DEV = 128
GROUP = 12
CACHE = 4096
N_SEQ = 32


def draw_hidden(key, part):
    first, second = jax.random.split(jax.random.fold_in(key, 11), 2)
    column = jnp.exp(jnp.log(10.0) * jnp.arange(D, dtype=jnp.float32) / (D - 1))
    rough = jax.random.uniform(second, (BATCH, D), jnp.float32, 0.7, 1.4)
    drawn = jnp.clip(jax.random.normal(first, (BATCH, D), jnp.float32), -5.0, 5.0)
    return jnp.clip(drawn * column * rough, -600.0, 600.0).astype(jnp.bfloat16)


def draw_lengths(key, part):
    first, second, third = jax.random.split(jax.random.fold_in(key, 23), 3)
    top_bits = CACHE.bit_length() - 1
    shifts = jnp.maximum(jax.random.randint(first, (BATCH,), -top_bits, top_bits + 1), 0)
    upper = jnp.right_shift(jnp.full((BATCH,), CACHE, jnp.int32), shifts.astype(jnp.int32))
    upper = jnp.maximum(upper, 1)
    drawn = jax.random.randint(second, (BATCH,), upper // 2 + 1, upper + 1)
    chosen = jax.random.randint(third, (), 0, BATCH)
    return jnp.where(jnp.arange(BATCH) == chosen, CACHE, drawn).astype(jnp.int32)


def draw_key_cache(key, part):
    first = jax.random.fold_in(jax.random.fold_in(key, 37), 0)
    drawn = 2.5 * jax.random.normal(first, (BATCH, KV_HEADS, CACHE, HD), jnp.float32)
    return jnp.clip(drawn, -15.0, 15.0).astype(jnp.bfloat16)


def level_of(rng, dims, shards, low, largest):
    def one(dim, shards_of):
        steps = jax.random.uniform(jax.random.fold_in(jax.random.fold_in(rng, 6), dim), (shards_of,), jnp.float32, low / len(shards), largest / len(shards))
        return jnp.repeat(jnp.exp(steps), dims[dim] // shards_of).reshape((-1,) + (1,) * (len(dims) - dim - 1))

    loudness = one(*shards[0])
    for cut in shards[1:]:
        loudness = loudness * one(*cut)
    return loudness


def normal_values(stream_key, dims, scale, reach, shards=(), held_as=jnp.bfloat16):
    values = scale * jax.random.normal(stream_key, dims, jnp.float32)
    if shards:
        values = values * level_of(stream_key, dims, shards, -0.22, 0.18)
    return jnp.clip(values, -reach, reach).astype(held_as)


def setup_inputs(seed: int = 0, part: int = 0) -> dict:
    keys = jax.random.split(jax.random.key(seed), 10)
    part_splits = jax.random.split(jax.random.fold_in(keys[9], part), 10)
    return {
        "hidden": draw_hidden(jax.random.fold_in(jax.random.fold_in(keys[9], part), 71), part),
        "norm_gain": jnp.clip(1.0 + 0.18 * jax.random.normal(keys[1], (D,), jnp.float32), 0.1, 1.9),
        "w_query": normal_values(keys[2], (D, HEADS * HD), D ** -0.5, 0.0546875, ((0, 32), (1, 8))),
        "w_key": normal_values(keys[3], (D, KV_HEADS * HD), D ** -0.5, 0.0546875, ((0, 32), (1, 8))),
        "w_value": normal_values(keys[4], (D, KV_HEADS * HD), D ** -0.5, 0.0546875, ((0, 32), (1, 8))),
        "w_out": normal_values(keys[5], (HEADS * HD, D), (HEADS * HD) ** -0.5, 0.0546875, ((0, 8), (1, 32))),
        "lengths": draw_lengths(jax.random.fold_in(jax.random.fold_in(keys[9], part), 71), part),
        "key_cache": draw_key_cache(jax.random.fold_in(jax.random.fold_in(keys[9], part), 71), part),
        "value_cache": normal_values(part_splits[8], (BATCH, KV_HEADS, CACHE, HD), 1.0, 6.0, ((1, 8), (2, 32))),
    }


EPSILON = 1e-05

def reference(hidden, norm_gain, w_query, w_key, w_value, w_out, lengths, key_cache, value_cache):
    widened = hidden.astype(jnp.float32)
    mean_square = lax.optimization_barrier(jnp.mean(widened * widened, axis=1, keepdims=True))
    inverse_rms = lax.rsqrt(mean_square + EPSILON)
    scaled = (widened * norm_gain).astype(jnp.bfloat16)
    query_full = jnp.dot(scaled, w_query, preferred_element_type=jnp.float32)
    queries = (query_full * inverse_rms * HD ** (-0.5)).astype(jnp.bfloat16)
    new_keys = (jnp.dot(scaled, w_key, preferred_element_type=jnp.float32) * inverse_rms).astype(jnp.bfloat16)
    new_values = (jnp.dot(scaled, w_value, preferred_element_type=jnp.float32) * inverse_rms).astype(jnp.bfloat16)
    grouped = queries.reshape(BATCH, KV_HEADS, GROUP, HD).transpose(1, 0, 2, 3)
    positions = jnp.arange(CACHE, dtype=jnp.int32)
    live_mask = positions[None, None, :] < lengths.astype(jnp.int32)[:, None, None]
    live_block = live_mask.reshape(BATCH, 1, N_SEQ, CTX_DEV)

    def per_head(operands):
        head_keys, head_values, head_query, new_key, new_value = operands
        scores = jnp.einsum('bgd,bpd->bgp', head_query.astype(jnp.float32), head_keys.astype(jnp.float32), precision=lax.Precision.HIGHEST)
        masked = jnp.where(live_mask, scores, -1e+30)
        blocked = masked.reshape(BATCH, GROUP, N_SEQ, CTX_DEV)
        block_max = lax.optimization_barrier(jnp.max(blocked, axis=-1))
        shifted = scores.reshape(BATCH, GROUP, N_SEQ, CTX_DEV) - block_max[..., None]
        weights = jnp.where(live_block, jnp.exp(jnp.where(live_block, shifted, 0.0)), 0.0).astype(jnp.bfloat16)
        block_den = lax.optimization_barrier(jnp.sum(weights.astype(jnp.float32), axis=-1))
        block_acc = jnp.einsum('bgcp,bcpd->bgcd', weights.astype(jnp.float32), head_values.reshape(BATCH, N_SEQ, CTX_DEV, HD).astype(jnp.float32), precision=lax.Precision.HIGHEST)
        self_score = lax.optimization_barrier(jnp.sum(head_query.astype(jnp.float32) * new_key.astype(jnp.float32)[:, None, :], axis=-1))
        top_score = jnp.maximum(lax.optimization_barrier(jnp.max(block_max, axis=-1)), self_score)
        factors = jnp.exp(block_max - top_score[..., None])
        own_weight = jnp.exp(self_score - top_score)
        denominator = lax.optimization_barrier(jnp.sum(factors * block_den, axis=-1)) + own_weight
        numerator = lax.optimization_barrier(jnp.sum(factors[..., None] * block_acc, axis=2)) + own_weight[..., None] * new_value.astype(jnp.float32)[:, None, :]
        return (numerator / denominator[..., None]).astype(jnp.bfloat16)
    attended = lax.map(per_head, (key_cache.transpose(1, 0, 2, 3), value_cache.transpose(1, 0, 2, 3), grouped, new_keys.reshape(BATCH, KV_HEADS, HD).transpose(1, 0, 2), new_values.reshape(BATCH, KV_HEADS, HD).transpose(1, 0, 2)))
    mixed = attended.transpose(1, 0, 2, 3).reshape(BATCH, HEADS * HD)
    return jnp.dot(mixed, w_out, preferred_element_type=jnp.float32).astype(jnp.bfloat16)
```

```python
import jax
import jax.numpy as jnp
from jax import lax
from jax.sharding import PartitionSpec as P

D = 12288
EPSILON = 1e-05


def exchange(x, axis):
    return lax.all_to_all(x, axis, split_axis=0, concat_axis=0, tiled=True)


def sent_to_all(x, axis):
    return exchange(jnp.broadcast_to(x, (lax.axis_size(axis), *x.shape)), axis)


def padded(x, rows):
    return jnp.pad(x, ((0, rows - x.shape[0]),) + ((0, 0),) * (x.ndim - 1))


def lane_row(x, lanes):
    return jnp.pad(x, ((0, 0), (0, lanes - x.shape[1])))[:, None, :]


def local(hidden, norm_gain, w_query, w_key, w_value, w_out, lengths, key_cache, value_cache):
    batch, _, block_len, hd = key_cache.shape
    group = w_query.shape[1] // hd
    peers = lax.axis_size("seq")
    me = lax.axis_index("seq")
    slots = group + 2
    half = batch // 2

    tokens = sent_to_all(hidden, "head").reshape(batch, hidden.shape[1])
    widened = tokens.astype(jnp.float32)
    squares = jnp.sum(widened * widened, axis=1)
    scaled = (widened * norm_gain).astype(jnp.bfloat16)

    def project(w):
        return jnp.dot(scaled, w, preferred_element_type=jnp.float32)

    q_part = project(w_query).reshape(batch, group, hd).transpose(1, 0, 2)
    parts = jnp.concatenate([q_part, project(w_key)[None], project(w_value)[None]], axis=0)
    parts = padded(parts.reshape(2 * slots, half, hd), peers)
    sq_rows = lane_row(jnp.tile(squares.reshape(2, half), (peers // 2, 1)), hd)
    sent = jnp.concatenate([parts, sq_rows], axis=1).reshape(peers, 1, (half + 1) * hd)
    total = exchange(sent, "seq").reshape(peers, half + 1, hd).sum(axis=0)
    inverse_rms = lax.rsqrt(total[half, :half] / D + EPSILON)[:, None]
    factor = jnp.where(me < 2 * group, jnp.float32(float(hd) ** -0.5), jnp.float32(1.0))
    rounded = (total[:half] * inverse_rms * factor).astype(jnp.bfloat16)
    rows = sent_to_all(rounded.reshape(1, half * hd), "seq").reshape(peers, half, hd)
    rows = rows[: 2 * slots].reshape(slots, batch, hd)
    queries = rows[:group].transpose(1, 0, 2)
    new_keys, new_values = rows[group], rows[group + 1]

    scores = jnp.einsum("bgd,bpd->bgp", queries, key_cache[:, 0], preferred_element_type=jnp.float32)
    positions = me * block_len + jnp.arange(block_len, dtype=jnp.int32)
    live = (positions[None, :] < lengths[:, None])[:, None, :]
    block_max = jnp.max(jnp.where(live, scores, -1e30), axis=-1)
    shifted = jnp.where(live, scores - block_max[..., None], 0.0)
    weights = jnp.where(live, jnp.exp(shifted), 0.0).astype(jnp.bfloat16)
    block_den = jnp.sum(weights.astype(jnp.float32), axis=-1)
    block_acc = jnp.einsum(
        "bgp,bpd->bgd", weights, value_cache[:, 0], preferred_element_type=jnp.float32
    )
    self_score = jnp.einsum("bgd,bd->bg", queries, new_keys, preferred_element_type=jnp.float32)
    self_score = jnp.where(me == 0, self_score, -1e30)
    top = jnp.maximum(block_max, self_score)
    keep = jnp.exp(block_max - top)
    own = jnp.where(me == 0, jnp.exp(self_score - top), 0.0)
    den = keep * block_den + own
    acc = keep[..., None] * block_acc + own[..., None] * new_values[:, None, :].astype(jnp.float32)

    share = batch * group // peers
    acc = acc.transpose(1, 0, 2).reshape(peers, share, hd)
    stats = jnp.concatenate([top.T.reshape(peers, share), den.T.reshape(peers, share)], axis=1)
    sent = jnp.concatenate([acc, lane_row(stats, hd)], axis=1).reshape(peers, 1, (share + 1) * hd)
    blocks = exchange(sent, "seq").reshape(peers, share + 1, hd)
    tops, dens = blocks[:, share, :share], blocks[:, share, share : 2 * share]
    factors = jnp.exp(tops - jnp.max(tops, axis=0))
    denominator = jnp.sum(factors * dens, axis=0)
    numerator = jnp.sum(factors[..., None] * blocks[:, :share], axis=0)
    mixed = (numerator / denominator[:, None]).astype(jnp.bfloat16)
    mixed = sent_to_all(mixed.reshape(1, share * hd), "seq").reshape(group, batch, hd)

    out = jnp.einsum(
        "gbd,gdn->bn", mixed, w_out.reshape(group, hd, -1), preferred_element_type=jnp.float32
    )
    ways = lax.axis_size("head")
    return exchange(out.reshape(ways, batch // ways, -1), "head").sum(axis=0).astype(jnp.bfloat16)


def solution(mesh):
    return jax.shard_map(
        local,
        mesh=mesh,
        in_specs=(
            P(("parts", "head"), "seq"),
            P("seq"),
            P("seq", "head"),
            P("seq", "head"),
            P("seq", "head"),
            P("head", "seq"),
            P("parts"),
            P("parts", "head", "seq", None),
            P("parts", "head", "seq", None),
        ),
        out_specs=P(("parts", "head"), "seq"),
        check_vma=False,
    )
```

```python
import jax
import jax.numpy as jnp
from jax import lax
from jax.sharding import PartitionSpec as P

D = 12288
EPSILON = 1e-05
NEAR = 4


def near_groups():
    peers = lax.axis_size("seq")
    return [[first + i for i in range(NEAR)] for first in range(0, peers, NEAR)]


def far_groups():
    peers = lax.axis_size("seq")
    return [list(range(first, peers, NEAR)) for first in range(NEAR)]


def exchange(x, axis, groups=None):
    return lax.all_to_all(
        x, axis, split_axis=0, concat_axis=0, tiled=True, axis_index_groups=groups
    )


def sent_to_all(x, axis, groups=None):
    ways = lax.axis_size(axis) if groups is None else len(groups[0])
    return exchange(jnp.broadcast_to(x, (ways, *x.shape)), axis, groups)


def to_rows(x, rows, lanes):
    return jnp.pad(x, ((0, 0), (0, rows - x.shape[1]), (0, lanes - x.shape[2])))


def fold(tops, dens, accs):
    top = jnp.max(tops, axis=0)
    factors = jnp.exp(tops - top)
    return top, jnp.sum(factors * dens, axis=0), jnp.sum(factors[..., None] * accs, axis=0)


def packed(top, den, acc):
    n, heads, batch, hd = acc.shape
    stats = jnp.concatenate([top, den], axis=1)
    return jnp.concatenate([acc.reshape(n, heads * batch, hd), to_rows(stats, 8, hd)], axis=1)


def unpacked(x, heads, batch):
    n, _, hd = x.shape
    acc = x[:, : heads * batch].reshape(n, heads, batch, hd)
    stats = x[:, heads * batch :, :batch]
    return stats[:, :heads], stats[:, heads : 2 * heads], acc


def local(hidden, norm_gain, w_query, w_key, w_value, w_out, lengths, key_cache, value_cache):
    batch, _, block_len, hd = key_cache.shape
    group = w_query.shape[1] // hd
    me = lax.axis_index("seq")
    near, far = near_groups(), far_groups()
    heads = group // NEAR
    piece = 2 * batch // NEAR
    main = heads * batch
    rows = main + piece + 4

    tokens = sent_to_all(hidden, "head").reshape(batch, hidden.shape[1])
    widened = tokens.astype(jnp.float32)
    squares = jnp.sum(widened * widened, axis=1)
    scaled = (widened * norm_gain).astype(jnp.bfloat16)

    def project(w):
        return jnp.dot(scaled, w, preferred_element_type=jnp.float32)

    q_part = project(w_query).reshape(batch, group, hd).transpose(1, 0, 2)
    kv_part = jnp.concatenate([project(w_key), project(w_value)], axis=0)
    sq_row = jnp.broadcast_to(squares, (NEAR, 1, batch))
    sent = jnp.concatenate(
        [q_part.reshape(NEAR, main, hd), kv_part.reshape(NEAR, piece, hd), to_rows(sq_row, 4, hd)],
        axis=1,
    )
    quarter = exchange(sent, "seq", near).sum(axis=0)
    total = sent_to_all(quarter, "seq", far).sum(axis=0)
    inverse_rms = lax.rsqrt(total[main + piece, :batch] / D + EPSILON)
    mine = lax.rem(me, NEAR)
    halves = inverse_rms.reshape(2, piece)
    kv_rms = jnp.where(lax.rem(mine, 2) == 0, halves[0], halves[1])
    queries = total[:main].reshape(heads, batch, hd) * inverse_rms[:, None] * float(hd) ** -0.5
    new_kv = total[main : main + piece] * kv_rms[:, None]
    rounded = jnp.concatenate(
        [queries.reshape(main, hd).astype(jnp.bfloat16), new_kv.astype(jnp.bfloat16)], axis=0
    )
    rounded = jnp.pad(rounded, ((0, rows - rounded.shape[0]), (0, 0)))
    gathered = sent_to_all(rounded, "seq", near)
    queries = gathered[:, :main].reshape(group, batch, hd).transpose(1, 0, 2)
    new_kv = gathered[:, main : main + piece].reshape(2, batch, hd)
    new_keys, new_values = new_kv[0], new_kv[1]

    scores = jnp.einsum("bgd,bpd->bgp", queries, key_cache[:, 0], preferred_element_type=jnp.float32)
    positions = me * block_len + jnp.arange(block_len, dtype=jnp.int32)
    live = (positions[None, :] < lengths[:, None])[:, None, :]
    block_max = jnp.max(jnp.where(live, scores, -1e30), axis=-1)
    shifted = jnp.where(live, scores - block_max[..., None], 0.0)
    weights = jnp.where(live, jnp.exp(shifted), 0.0).astype(jnp.bfloat16)
    block_den = jnp.sum(weights.astype(jnp.float32), axis=-1)
    block_acc = jnp.einsum(
        "bgp,bpd->bgd", weights, value_cache[:, 0], preferred_element_type=jnp.float32
    )
    self_score = jnp.einsum("bgd,bd->bg", queries, new_keys, preferred_element_type=jnp.float32)
    self_score = jnp.where(me == 0, self_score, -1e30)
    top = jnp.maximum(block_max, self_score)
    keep = jnp.exp(block_max - top)
    own = jnp.where(me == 0, jnp.exp(self_score - top), 0.0)
    den = keep * block_den + own
    acc = keep[..., None] * block_acc + own[..., None] * new_values[:, None, :].astype(jnp.float32)

    split = (NEAR, heads, batch)
    sent = packed(
        top.T.reshape(split), den.T.reshape(split), acc.transpose(1, 0, 2).reshape(*split, hd)
    )
    top, den, acc = fold(*unpacked(exchange(sent, "seq", near), heads, batch))
    quarter = packed(top[None], den[None], acc[None])[0]
    _, den, acc = fold(*unpacked(sent_to_all(quarter, "seq", far), heads, batch))
    mixed = (acc / den[..., None]).astype(jnp.bfloat16).reshape(main, hd)
    mixed = sent_to_all(mixed, "seq", near).reshape(group, batch, hd)

    out = jnp.einsum(
        "gbd,gdn->bn", mixed, w_out.reshape(group, hd, -1), preferred_element_type=jnp.float32
    )
    ways = lax.axis_size("head")
    return exchange(out.reshape(ways, batch // ways, -1), "head").sum(axis=0).astype(jnp.bfloat16)


def solution(mesh):
    return jax.shard_map(
        local,
        mesh=mesh,
        in_specs=(
            P(("parts", "head"), "seq"),
            P("seq"),
            P("seq", "head"),
            P("seq", "head"),
            P("seq", "head"),
            P("head", "seq"),
            P("parts"),
            P("parts", "head", "seq", None),
            P("parts", "head", "seq", None),
        ),
        out_specs=P(("parts", "head"), "seq"),
        check_vma=False,
    )
```
